768 devices in a mesh: fsdp: 48 (over x, z), grp: 16 (over y, core).
Axes of the slice: x: 4, y: 8, z: 12, core: 2. Of those that a mesh axis runs over, the one named last changes fastest.
Arguments:
- gradient: bfloat16 [768, 512, 512], P('fsdp', 'grp'), may hold values from -6 to 6
- left_factor: bfloat16 [2304, 512, 512], P(('fsdp', 'grp'))
- right_factor: bfloat16 [2304, 512, 512], P(('fsdp', 'grp'))
- block_owner: int32 [768], replicated, may hold values from 0 to 767, as said below
Outputs:
- preconditioned: bfloat16 [768, 512, 512], P('fsdp', 'grp')
The draws below stay inside these ranges and needn't reach their ends.
Inputs may be any that keep to these rules, and one draw needn't show every extreme that they name: block_owner[b] is a device index, fsdp index times 16 plus grp index. The 16 blocks homed at one fsdp index go to devices of 16 different fsdp indices; the devices of each fsdp index own 16 blocks in all; no device owns more than 3 blocks, and at every fsdp index one device owns exactly 3.
All inputs are finite; a program needn't handle non-finite values.
Results may differ from the reference program's by a relative error of at most 0.0049.
Values may be sent and summed in bfloat16 or wider, within the bound.
No kernel may reach another device: no remote copies, remote signals or barrier semaphores. Data moves between devices by JAX's collectives and lax.ppermute only.
A program may use at most 32 MiB of HBM per device.

```python
import jax
import jax.numpy as jnp
from jax import lax

B = 512
CAP = 3
BLOCKS_COL = 16
BLOCKS = 768
N_FSDP = 48
N_GRP = 16


def draw_factor_common(key, salt_value):
    key_diag, key_noise = jax.random.split(jax.random.fold_in(key, salt_value))
    count = N_FSDP * N_GRP * CAP
    diagonal = jax.random.uniform(key_diag, (count, B), jnp.float32, 0.5, 1.5)
    noise = jax.random.normal(key_noise, (count, B, B), jnp.float32) * (0.5 / B ** 0.5)
    identity = jnp.eye(B, dtype=jnp.float32)
    return noise + diagonal[:, :, None] * identity[None, :, :]


def draw_left_factor(key, part):
    return draw_factor_common(key, 21).astype(jnp.bfloat16)


def draw_right_factor(key, part):
    return draw_factor_common(key, 37).astype(jnp.bfloat16)


def draw_block_owner(key, part):
    key_offsets, key_full, key_order = jax.random.split(jax.random.fold_in(key, 11), 3)
    offsets = jax.random.permutation(key_offsets, N_FSDP)[:BLOCKS_COL].astype(jnp.int32)
    halfway = N_FSDP // 2
    has_half = jnp.any(offsets == halfway)
    offsets = offsets.at[0].set(jnp.where(has_half, offsets[0], halfway)).astype(jnp.int32)
    column_ids = jnp.arange(N_FSDP, dtype=jnp.int32)
    dest_column = (column_ids[:, None] + offsets[None, :]) % N_FSDP
    source_column = (column_ids[:, None] - offsets[None, :]) % N_FSDP
    arrival_rank = jnp.sum(source_column[:, None, :] < source_column[:, :, None], axis=2).astype(jnp.int32)
    full_owner = jax.random.randint(key_full, (N_FSDP,), 0, N_GRP)
    spare_slots = N_GRP * CAP - CAP
    priority = jax.random.randint(key_order, (N_FSDP, spare_slots), 0, 1 << 20) * spare_slots + jnp.arange(spare_slots, dtype=jnp.int32)[None, :]
    spare_order = jnp.argsort(priority, axis=1).astype(jnp.int32)
    later_owner = jnp.take_along_axis(spare_order, jnp.clip(arrival_rank - CAP, 0, spare_slots - 1), axis=1) // CAP
    later_owner = later_owner + (later_owner >= full_owner[:, None]).astype(jnp.int32)
    owner_group = jnp.where(arrival_rank < CAP, full_owner[:, None], later_owner)
    picked = owner_group[dest_column, jnp.arange(BLOCKS_COL, dtype=jnp.int32)[None, :]]
    return (dest_column * N_GRP + picked).reshape(-1).astype(jnp.int32)


def shard_levels(rng, shape, cuts, low, top_value):
    def one(axis_at, shards_of):
        heights = jax.random.uniform(jax.random.fold_in(jax.random.fold_in(rng, 6), axis_at), (shards_of,), jnp.float32, low / len(cuts), top_value / len(cuts))
        return jnp.repeat(jnp.exp(heights), shape[axis_at] // shards_of).reshape((-1,) + (1,) * (len(shape) - axis_at - 1))

    level = one(*cuts[0])
    for cut in cuts[1:]:
        level = level * one(*cut)
    return level


def bell_draw(own_key, extent, spread, limit, cuts=(), held_as=jnp.bfloat16):
    entries = jax.random.normal(own_key, extent, jnp.float32) * spread
    if len(cuts) > 0:
        entries = shard_levels(own_key, extent, cuts, -0.22, 0.18) * entries
    return jnp.clip(entries, min=-limit, max=limit).astype(held_as)


def setup_inputs(seed: int = 0) -> dict:
    streams_of = jax.random.split(jax.random.key(seed), 5)
    return {
        "gradient": bell_draw(streams_of[0], (BLOCKS, B, B), 1.0, 6.0, ((0, 48), (1, 16))),
        "left_factor": draw_left_factor(jax.random.fold_in(streams_of[4], 71), 0),
        "right_factor": draw_right_factor(jax.random.fold_in(streams_of[4], 71), 0),
        "block_owner": draw_block_owner(jax.random.fold_in(streams_of[4], 71), 0),
    }


def reference(gradient, left_factor, right_factor, block_owner):
    block_ids = jnp.arange(BLOCKS, dtype=jnp.int32)
    earlier = (block_owner[None, :] == block_owner[:, None]) & (block_ids[None, :] < block_ids[:, None])
    slot_index = (block_owner + 0).astype(jnp.int32) * CAP + jnp.sum(earlier, axis=1).astype(jnp.int32)

    def precondition_group(packed):
        grad_group, indices = packed
        left_group = jnp.take(left_factor, indices, axis=0).astype(jnp.float32)
        right_group = jnp.take(right_factor, indices, axis=0).astype(jnp.float32)
        product = jnp.einsum("kab,kbc->kac", left_group, grad_group.astype(jnp.float32)).astype(jnp.bfloat16)
        return jnp.einsum("kab,kbc->kac", product.astype(jnp.float32), right_group).astype(jnp.bfloat16)

    grouped = gradient.reshape(BLOCKS // BLOCKS_COL, BLOCKS_COL, B, B)
    indices_grouped = slot_index.reshape(BLOCKS // BLOCKS_COL, BLOCKS_COL).astype(jnp.int32)
    stacked = lax.map(precondition_group, (grouped, indices_grouped))
    return stacked.reshape(BLOCKS, B, B)
```

```python
import jax
import jax.numpy as jnp
from jax import lax
from jax.experimental import pallas as pl
from jax.experimental.pallas import tpu as pltpu
from jax.sharding import PartitionSpec as P

VMEM = pltpu.VMEM
SMEM = pltpu.SMEM


def place_kernel(table, source, out):
    for i in range(source.shape[0]):
        out[table[i]] = source[i]


def place_live_kernel(table, source, out):
    def step(i, carry):
        @pl.when(table[i] >= 0)
        def _():
            out[table[i]] = source[i]

        return carry

    lax.fori_loop(0, source.shape[0], step, 0)


def fetch_live_kernel(table, source, out):
    def step(i, carry):
        @pl.when(table[i] >= 0)
        def _():
            out[i] = source[table[i]]

        return carry

    lax.fori_loop(0, out.shape[0], step, 0)


def fetch_kernel(table, source, out):
    for i in range(out.shape[0]):
        out[i] = source[table[i]]


def moved(kernel, table, source, pieces, name, resident=True):
    if resident:
        source = pltpu.with_memory_space_constraint(source, VMEM)
    return pl.pallas_call(
        kernel,
        out_shape=VMEM((pieces, *source.shape[1:]), source.dtype),
        in_specs=[pl.BlockSpec(memory_space=SMEM), pl.BlockSpec(memory_space=VMEM)],
        out_specs=pl.BlockSpec(memory_space=VMEM),
        name=name,
        compiler_params=pltpu.CompilerParams(vmem_limit_bytes=4 << 20),
    )(table, source)


def product_kernel(left, blocks, right, out):
    slots, size, _ = left.shape
    for k in range(slots):
        block = blocks[:, k].reshape(size, size)
        half = jnp.dot(left[k], block, preferred_element_type=jnp.float32).astype(left.dtype)
        full = jnp.dot(half, right[k], preferred_element_type=jnp.float32).astype(left.dtype)
        out[:, k] = full.reshape(out.shape[0], *out.shape[2:])


def products(left, blocks, right):
    slots, size, _ = left.shape
    resident = pl.BlockSpec(memory_space=VMEM)
    return pl.pallas_call(
        product_kernel,
        out_shape=VMEM(blocks.shape, blocks.dtype),
        in_specs=[resident, resident, resident],
        out_specs=resident,
        name="products",
        compiler_params=pltpu.CompilerParams(vmem_limit_bytes=16 << 20),
        cost_estimate=pl.CostEstimate(
            flops=4 * slots * size**3, transcendentals=0, bytes_accessed=2 * (2 * left.size + 2 * blocks.size)
        ),
    )(*(pltpu.with_memory_space_constraint(x, VMEM) for x in (left, blocks, right)))


def exchanged(pieces, axis):
    return lax.all_to_all(pieces, axis, split_axis=0, concat_axis=0, tiled=True)


def per_device(gradient, left_factor, right_factor, block_owner):
    local_blocks, rows, width = gradient.shape
    slots = left_factor.shape[0]
    columns = lax.axis_size("fsdp")
    groups = lax.axis_size("grp")
    column = lax.axis_index("fsdp")
    mine = lax.dynamic_slice_in_dim(block_owner, column * local_blocks, local_blocks) // groups
    outgoing = moved(place_kernel, mine, gradient, columns, "to_columns", False)
    arrived = exchanged(outgoing, "fsdp")
    owners = block_owner.reshape(columns, local_blocks)
    toward = owners // groups == column
    live = jnp.any(toward, axis=1)
    target = jnp.sum(jnp.where(toward, owners % groups, 0), axis=1)
    ids = jnp.arange(columns, dtype=jnp.int32)
    earlier = (target[None, :] == target[:, None]) & live[None, :] & (ids[None, :] < ids[:, None])
    rank = jnp.sum(earlier.astype(jnp.int32), axis=1)
    slot = jnp.where(live, target * slots + rank, -1).astype(jnp.int32)
    packed = moved(place_live_kernel, slot, arrived, groups * slots, "to_slots")
    blocks = exchanged(packed.reshape(groups, slots, rows, width), "grp")
    result = products(left_factor, blocks, right_factor)
    returned = exchanged(result, "grp").reshape(groups * slots, rows, width)
    homeward = moved(fetch_live_kernel, slot, returned, columns, "from_slots")
    home = exchanged(homeward, "fsdp")
    return moved(fetch_kernel, mine, home, local_blocks, "from_columns")


def solution(mesh):
    placed = (P("fsdp", "grp", None), P(("fsdp", "grp"), None, None), P(("fsdp", "grp"), None, None), P())
    return jax.shard_map(
        per_device, mesh=mesh, in_specs=placed, out_specs=P("fsdp", "grp", None), check_vma=False
    )
```

```python
import jax
import jax.numpy as jnp
from jax import lax
from jax.experimental import pallas as pl
from jax.experimental.pallas import tpu as pltpu
from jax.sharding import PartitionSpec as P

HBM = pltpu.HBM
VMEM = pltpu.VMEM
SMEM = pltpu.SMEM


def place_kernel(table, source, out):
    for i in range(source.shape[0]):
        out[table[i]] = source[i]


def place_live_kernel(table, source, out):
    def step(i, carry):
        @pl.when(table[i] >= 0)
        def _():
            out[table[i]] = source[i]

        return carry

    lax.fori_loop(0, source.shape[0], step, 0)


def fetch_live_kernel(table, source, out):
    def step(i, carry):
        @pl.when(table[i] >= 0)
        def _():
            out[i] = source[table[i]]

        return carry

    lax.fori_loop(0, out.shape[0], step, 0)


def fetch_kernel(table, source, out):
    for i in range(out.shape[0]):
        out[i] = source[table[i]]


def moved(kernel, table, source, pieces, name, resident=True):
    if resident:
        source = pltpu.with_memory_space_constraint(source, VMEM)
    return pl.pallas_call(
        kernel,
        out_shape=VMEM((pieces, *source.shape[1:]), source.dtype),
        in_specs=[pl.BlockSpec(memory_space=SMEM), pl.BlockSpec(memory_space=VMEM)],
        out_specs=pl.BlockSpec(memory_space=VMEM),
        name=name,
        compiler_params=pltpu.CompilerParams(vmem_limit_bytes=4 << 20),
    )(table, source)


def split_kernel(start, left, right, *rest):
    pieces, arrivals = rest[:-1], rest[-1]
    count = len(pieces)
    rows = pieces[0].shape[1]
    last = left.shape[0] - 1
    copies = []
    for d in range(count):
        first = pl.multiple_of(lax.rem(start[0] + d, count) * rows, rows)
        for side, factor in enumerate((left, right)):
            copies.append(
                pltpu.make_async_copy(
                    factor.at[last, pl.ds(first, rows)], pieces[d].at[side], arrivals.at[2 * d + side]
                )
            )
    for copy in copies:
        copy.start()
    for copy in copies:
        copy.wait()


def split_factors(start, left, right, count):
    size = left.shape[-1]
    piece = HBM((2, size // count, size), left.dtype)
    hbm = pl.BlockSpec(memory_space=HBM)
    return pl.pallas_call(
        split_kernel,
        out_shape=[piece] * count,
        in_specs=[pl.BlockSpec(memory_space=SMEM), hbm, hbm],
        out_specs=[hbm] * count,
        scratch_shapes=[pltpu.SemaphoreType.DMA((2 * count,))],
        name="split_factors",
        compiler_params=pltpu.CompilerParams(vmem_limit_bytes=1 << 20),
    )(start, *(pltpu.with_memory_space_constraint(x, HBM) for x in (left, right)))


def select_kernel(table, near, far, *pieces):
    count = near.shape[0]
    for d, piece in enumerate(pieces):

        @pl.when((table[d] >= 0) & (table[d] < count))
        def _():
            piece[...] = near[table[d]]

        @pl.when(table[d] >= count)
        def _():
            piece[...] = far[table[d] - count]


def select_shares(table, near, far):
    resident = pl.BlockSpec(memory_space=VMEM)
    count = near.shape[0]
    return pl.pallas_call(
        select_kernel,
        out_shape=[VMEM(near.shape[1:], near.dtype)] * count,
        in_specs=[pl.BlockSpec(memory_space=SMEM), resident, resident],
        out_specs=[resident] * count,
        name="select_shares",
        compiler_params=pltpu.CompilerParams(vmem_limit_bytes=4 << 20),
    )(table, *(pltpu.with_memory_space_constraint(x, VMEM) for x in (near, far)))


def product_kernel(place, left, right, blocks, *rest):
    shares, out, factors = rest[:-2], rest[-2], rest[-1]
    size = left.shape[-1]
    slots = out.shape[1]
    count = len(shares)
    rows = size // count

    def product(k, left_matrix, right_matrix):
        block = blocks[:, k].reshape(size, size)
        half = jnp.dot(left_matrix, block, preferred_element_type=jnp.float32).astype(left.dtype)
        full = jnp.dot(half, right_matrix, preferred_element_type=jnp.float32).astype(left.dtype)
        out[:, k] = full.reshape(out.shape[0], *out.shape[2:])

    @pl.when(place[1] == 0)
    def _():
        factors[0] = left[slots - 1]
        factors[1] = right[slots - 1]

    @pl.when(place[1] != 0)
    def _():
        for d, share in enumerate(shares):
            first = pl.multiple_of(lax.rem(place[0] + count - d, count) * rows, rows)
            for side in range(2):
                factors[side, pl.ds(first, rows), :] = share[side]

    for k in range(slots - 1):
        product(k, left[k], right[k])
    product(slots - 1, factors[0], factors[1])


def products(place, left, right, blocks, shares):
    slots = blocks.shape[1]
    size = left.shape[-1]
    resident = pl.BlockSpec(memory_space=VMEM)
    operands = (left, right, blocks, *shares)
    return pl.pallas_call(
        product_kernel,
        out_shape=VMEM(blocks.shape, blocks.dtype),
        in_specs=[pl.BlockSpec(memory_space=SMEM)] + [resident] * len(operands),
        out_specs=resident,
        scratch_shapes=[VMEM((2, size, size), left.dtype)],
        name="products",
        compiler_params=pltpu.CompilerParams(vmem_limit_bytes=16 << 20),
        cost_estimate=pl.CostEstimate(
            flops=4 * slots * size**3, transcendentals=0, bytes_accessed=4 * (left.size + blocks.size)
        ),
    )(place, *(pltpu.with_memory_space_constraint(x, VMEM) for x in operands))


def shifted(pieces, ring):
    devices = ring * 2
    return pieces[:1] + [
        lax.ppermute(pieces[d], "grp", [(i, (i + 2 * d) % devices) for i in range(devices)]) for d in range(1, ring)
    ]


def exchanged(pieces, axis):
    return lax.all_to_all(pieces, axis, split_axis=0, concat_axis=0, tiled=True)


def per_device(gradient, left_factor, right_factor, block_owner):
    local_blocks, rows, width = gradient.shape
    slots = left_factor.shape[0] - 1
    columns = lax.axis_size("fsdp")
    groups = lax.axis_size("grp")
    ring = groups // 2
    column = lax.axis_index("fsdp")
    group = lax.axis_index("grp")
    chip, core = group // 2, group % 2
    mine = lax.dynamic_slice_in_dim(block_owner, column * local_blocks, local_blocks) // groups
    outgoing = moved(place_kernel, mine, gradient, columns, "to_columns", False)
    arrived = exchanged(outgoing, "fsdp")
    owners = block_owner.reshape(columns, local_blocks)
    toward = owners // groups == column
    live = jnp.any(toward, axis=1)
    target = jnp.sum(jnp.where(toward, owners % groups, 0), axis=1)
    ids = jnp.arange(columns, dtype=jnp.int32)
    earlier = (target[None, :] == target[:, None]) & live[None, :] & (ids[None, :] < ids[:, None])
    rank = jnp.sum(earlier.astype(jnp.int32), axis=1)
    members = jnp.arange(groups, dtype=jnp.int32)
    owned = jnp.sum(((target[None, :] == members[:, None]) & live[None, :]).astype(jnp.int32), axis=1)
    over = owned > slots
    spare = owned < slots
    below = members[None, :] < members[:, None]
    over_rank = jnp.sum((over[None, :] & below).astype(jnp.int32), axis=1)
    spare_rank = jnp.sum((spare[None, :] & below).astype(jnp.int32), axis=1)
    helps = over[:, None] & spare[None, :] & (over_rank[:, None] == spare_rank[None, :])
    helper = jnp.sum(jnp.where(helps, members[None, :], 0), axis=1)
    helped = jnp.sum(jnp.where(helps, members[:, None] + 1, 0), axis=0) - 1
    target_helper = jnp.sum(jnp.where(target[:, None] == members[None, :], helper[None, :], 0), axis=1)
    slot = jnp.where(rank < slots, target * slots + rank, target_helper * slots + slots - 1)
    slot = jnp.where(live, slot, -1).astype(jnp.int32)
    shares = shifted(list(split_factors(chip.reshape(1).astype(jnp.int32), left_factor, right_factor, ring)), ring)
    near = jnp.stack(shares)
    far = lax.ppermute(near, "grp", [(i, i ^ 1) for i in range(groups)])
    onward = (jnp.arange(ring, dtype=jnp.int32) + chip) % ring * 2 + core
    from_member = jnp.sum(jnp.where(onward[:, None] == members[None, :], helped[None, :], 0), axis=1)
    away = (chip - from_member // 2 + ring) % ring
    other = (from_member % 2 != core).astype(jnp.int32)
    table = jnp.where(from_member >= 0, away + other * ring, -1).astype(jnp.int32)
    shares = shifted(list(select_shares(table, near, far)), ring)
    helping = jnp.sum(jnp.where(members == group, helped, 0)) >= 0
    place = jnp.stack([chip.astype(jnp.int32), helping.astype(jnp.int32)])

    packed = moved(place_live_kernel, slot, arrived, groups * slots, "to_slots")
    packed, place, *shares = lax.optimization_barrier((packed, place, *shares))
    blocks = exchanged(packed.reshape(groups, slots, rows, width), "grp")
    result = products(place, left_factor, right_factor, blocks, shares)
    returned = exchanged(result, "grp").reshape(groups * slots, rows, width)
    homeward = moved(fetch_live_kernel, slot, returned, columns, "from_slots")
    home = exchanged(homeward, "fsdp")
    return moved(fetch_kernel, mine, home, local_blocks, "from_columns")


def solution(mesh):
    placed = (P("fsdp", "grp", None), P(("fsdp", "grp"), None, None), P(("fsdp", "grp"), None, None), P())
    return jax.shard_map(
        per_device, mesh=mesh, in_specs=placed, out_specs=P("fsdp", "grp", None), check_vma=False
    )
```

```python
import functools

import jax
import jax.numpy as jnp
from jax import lax
from jax.experimental import pallas as pl
from jax.experimental.pallas import tpu as pltpu
from jax.sharding import PartitionSpec as P

HBM = pltpu.HBM
VMEM = pltpu.VMEM
SMEM = pltpu.SMEM


def place_kernel(table, source, out):
    for i in range(source.shape[0]):
        out[table[i]] = source[i]


def place_live_kernel(table, source, out):
    def step(i, carry):
        @pl.when(table[i] >= 0)
        def _():
            out[table[i]] = source[i]

        return carry

    lax.fori_loop(0, source.shape[0], step, 0)


def fetch_live_kernel(table, source, out):
    def step(i, carry):
        @pl.when(table[i] >= 0)
        def _():
            out[i] = source[table[i]]

        return carry

    lax.fori_loop(0, out.shape[0], step, 0)


def fetch_kernel(table, source, out):
    for i in range(out.shape[0]):
        out[i] = source[table[i]]


def moved(kernel, table, source, pieces, name, resident=True):
    if resident:
        source = pltpu.with_memory_space_constraint(source, VMEM)
    return pl.pallas_call(
        kernel,
        out_shape=VMEM((pieces, *source.shape[1:]), source.dtype),
        in_specs=[pl.BlockSpec(memory_space=SMEM), pl.BlockSpec(memory_space=VMEM)],
        out_specs=pl.BlockSpec(memory_space=VMEM),
        name=name,
        compiler_params=pltpu.CompilerParams(vmem_limit_bytes=4 << 20),
    )(table, source)


OFFERS = ((0, 1), (-1, 0), (-1, 1), (1, 0), (1, 1), (-2, 0), (-2, 1), (2, 0), (2, 1))
REACH = (0, -1, 1, -2, 2)


def match_kernel(owned, helper, helped, *, slots):
    groups = owned.shape[0]
    ring = groups // 2
    for g in range(groups):
        helper[g] = jnp.int32(0)
        helped[g] = jnp.where(owned[g] < slots, -1, -2).astype(jnp.int32)

    def step(g, carry):
        chip = lax.div(g, jnp.int32(2))
        core = lax.rem(g, jnp.int32(2))
        need = jnp.where(owned[g] > slots, 1, 0).astype(jnp.int32)
        for chips, swap in OFFERS:
            offer = lax.rem(chip + (chips + ring), jnp.int32(ring)) * 2 + (1 - core if swap else core)
            free = jnp.where(helped[offer] == -1, 1, 0).astype(jnp.int32)

            @pl.when(need * free > 0)
            def _():
                helped[offer] = g
                helper[g] = offer

            need = need * (1 - free)
        return carry

    lax.fori_loop(jnp.int32(0), jnp.int32(groups), step, jnp.int32(0))


def matched(owned, slots):
    scalars = pl.BlockSpec(memory_space=SMEM)
    table = jax.ShapeDtypeStruct(owned.shape, jnp.int32)
    return pl.pallas_call(
        functools.partial(match_kernel, slots=slots),
        out_shape=[table, table],
        in_specs=[scalars],
        out_specs=[scalars, scalars],
        name="match",
        compiler_params=pltpu.CompilerParams(vmem_limit_bytes=1 << 20),
    )(owned)


def last_kernel(left, right, out, arrivals):
    last = left.shape[0] - 1
    copies = [
        pltpu.make_async_copy(factor.at[last], out.at[side], arrivals.at[side])
        for side, factor in enumerate((left, right))
    ]
    for copy in copies:
        copy.start()
    for copy in copies:
        copy.wait()


def last_factors(left, right):
    hbm = pl.BlockSpec(memory_space=HBM)
    return pl.pallas_call(
        last_kernel,
        out_shape=VMEM((2, *left.shape[1:]), left.dtype),
        in_specs=[hbm, hbm],
        out_specs=pl.BlockSpec(memory_space=VMEM),
        scratch_shapes=[pltpu.SemaphoreType.DMA((2,))],
        name="last_factors",
        compiler_params=pltpu.CompilerParams(vmem_limit_bytes=4 << 20),
    )(*(pltpu.with_memory_space_constraint(x, HBM) for x in (left, right)))


def select_kernel(table, *rest):
    candidates, outs = rest[:-2], rest[-2:]
    for k, out in enumerate(outs):
        for index, candidate in enumerate(candidates):

            @pl.when(table[k] == index)
            def _():
                out[...] = candidate[...]


def selected(table, candidates):
    resident = pl.BlockSpec(memory_space=VMEM)
    out = VMEM(candidates[0].shape, candidates[0].dtype)
    return pl.pallas_call(
        select_kernel,
        out_shape=[out, out],
        in_specs=[pl.BlockSpec(memory_space=SMEM)] + [resident] * len(candidates),
        out_specs=[resident, resident],
        name="select",
        compiler_params=pltpu.CompilerParams(vmem_limit_bytes=16 << 20),
    )(table, *(pltpu.with_memory_space_constraint(x, VMEM) for x in candidates))


def product_kernel(source, left, right, blocks, near, far, out):
    size = left.shape[-1]
    slots = out.shape[1]

    def product(k, left_matrix, right_matrix):
        block = blocks[:, k].reshape(size, size)
        half = jnp.dot(left_matrix, block, preferred_element_type=jnp.float32).astype(left.dtype)
        full = jnp.dot(half, right_matrix, preferred_element_type=jnp.float32).astype(left.dtype)
        out[:, k] = full.reshape(out.shape[0], *out.shape[2:])

    for k in range(slots - 1):
        product(k, left[k], right[k])
    last = slots - 1

    @pl.when(source[0] == 0)
    def _():
        product(last, left[last], right[last])

    @pl.when(source[0] == 1)
    def _():
        product(last, near[0], near[1])

    @pl.when(source[0] == 2)
    def _():
        product(last, far[0], far[1])


def products(source, left, right, blocks, near, far):
    slots = blocks.shape[1]
    size = left.shape[-1]
    resident = pl.BlockSpec(memory_space=VMEM)
    operands = (left, right, blocks, near, far)
    return pl.pallas_call(
        product_kernel,
        out_shape=VMEM(blocks.shape, blocks.dtype),
        in_specs=[pl.BlockSpec(memory_space=SMEM)] + [resident] * len(operands),
        out_specs=resident,
        name="products",
        compiler_params=pltpu.CompilerParams(vmem_limit_bytes=16 << 20),
        cost_estimate=pl.CostEstimate(
            flops=4 * slots * size**3, transcendentals=0, bytes_accessed=4 * (left.size + blocks.size)
        ),
    )(source, *(pltpu.with_memory_space_constraint(x, VMEM) for x in operands))


def shifted(array, step, size):
    return lax.ppermute(array, "grp", [(i, (i + step) % size) for i in range(size)])


def exchanged(pieces, axis):
    return lax.all_to_all(pieces, axis, split_axis=0, concat_axis=0, tiled=True)


def per_device(gradient, left_factor, right_factor, block_owner):
    local_blocks, rows, width = gradient.shape
    slots = left_factor.shape[0] - 1
    columns = lax.axis_size("fsdp")
    groups = lax.axis_size("grp")
    ring = groups // 2
    column = lax.axis_index("fsdp")
    group = lax.axis_index("grp")
    chip, core = group // 2, group % 2
    mine = lax.dynamic_slice_in_dim(block_owner, column * local_blocks, local_blocks) // groups
    outgoing = moved(place_kernel, mine, gradient, columns, "to_columns", False)
    arrived = exchanged(outgoing, "fsdp")
    owners = block_owner.reshape(columns, local_blocks)
    toward = owners // groups == column
    live = jnp.any(toward, axis=1)
    target = jnp.sum(jnp.where(toward, owners % groups, 0), axis=1)
    ids = jnp.arange(columns, dtype=jnp.int32)
    earlier = (target[None, :] == target[:, None]) & live[None, :] & (ids[None, :] < ids[:, None])
    rank = jnp.sum(earlier.astype(jnp.int32), axis=1)
    members = jnp.arange(groups, dtype=jnp.int32)
    owned = jnp.sum(((target[None, :] == members[:, None]) & live[None, :]).astype(jnp.int32), axis=1)
    helper, helped = matched(owned, slots)
    target_helper = jnp.sum(jnp.where(target[:, None] == members[None, :], helper[None, :], 0), axis=1)
    slot = jnp.where(rank < slots, target * slots + rank, target_helper * slots + slots - 1)
    slot = jnp.where(live, slot, -1).astype(jnp.int32)
    own = last_factors(left_factor, right_factor)
    below = shifted(own, 2, groups)
    above = shifted(own, -2, groups)
    candidates = (own, below, above, shifted(below, 2, groups), shifted(above, -2, groups))
    pair = jnp.stack([group, group ^ 1])
    giver = jnp.sum(jnp.where(pair[:, None] == members[None, :], helped[None, :], 0), axis=1)
    away = (giver // 2 - chip + ring) % ring
    reach = jnp.array(REACH, dtype=jnp.int32) % ring
    index = jnp.sum(jnp.where(away[:, None] == reach[None, :], jnp.arange(len(REACH))[None, :], 0), axis=1)
    here = (giver >= 0) & (giver % 2 == core)
    table = jnp.where(here, index, -1).astype(jnp.int32)
    source = jnp.where(giver[:1] < 0, 0, jnp.where(here[:1], 1, 2)).astype(jnp.int32)
    near, passed = selected(table, candidates)

    packed = moved(place_live_kernel, slot, arrived, groups * slots, "to_slots")
    packed, source, near, passed = lax.optimization_barrier((packed, source, near, passed))
    far = lax.ppermute(passed, "grp", [(i, i ^ 1) for i in range(groups)])
    blocks = exchanged(packed.reshape(groups, slots, rows, width), "grp")
    result = products(source, left_factor, right_factor, blocks, near, far)
    returned = exchanged(result, "grp").reshape(groups * slots, rows, width)
    homeward = moved(fetch_live_kernel, slot, returned, columns, "from_slots")
    home = exchanged(homeward, "fsdp")
    return moved(fetch_kernel, mine, home, local_blocks, "from_columns")


def solution(mesh):
    placed = (P("fsdp", "grp", None), P(("fsdp", "grp"), None, None), P(("fsdp", "grp"), None, None), P())
    return jax.shard_map(
        per_device, mesh=mesh, in_specs=placed, out_specs=P("fsdp", "grp", None), check_vma=False
    )
```

```python
import functools

import jax
import jax.numpy as jnp
from jax import lax
from jax.experimental import pallas as pl
from jax.experimental.pallas import tpu as pltpu
from jax.sharding import PartitionSpec as P

HBM = pltpu.HBM
VMEM = pltpu.VMEM
SMEM = pltpu.SMEM


def run(copies):
    for copy in copies:
        copy.start()
    for copy in copies:
        copy.wait()


def to_columns_kernel(column, owner, source, out, owners, pieces, loads, stores, *, groups):
    run(
        [
            pltpu.make_async_copy(owner, owners, loads.at[0]),
            pltpu.make_async_copy(source, pieces, loads.at[1]),
        ]
    )
    run(
        [
            pltpu.make_async_copy(
                pieces.at[i],
                out.at[lax.div(owners[column[0] * source.shape[0] + i], jnp.int32(groups))],
                stores.at[i],
            )
            for i in range(source.shape[0])
        ]
    )


def to_columns(column, owner, source, columns, groups):
    hbm = pl.BlockSpec(memory_space=HBM)
    return pl.pallas_call(
        functools.partial(to_columns_kernel, groups=groups),
        out_shape=HBM((columns, *source.shape[1:]), source.dtype),
        in_specs=[pl.BlockSpec(memory_space=SMEM), hbm, hbm],
        out_specs=hbm,
        scratch_shapes=[
            SMEM(owner.shape, owner.dtype),
            VMEM(source.shape, source.dtype),
            pltpu.SemaphoreType.DMA((2,)),
            pltpu.SemaphoreType.DMA((source.shape[0],)),
        ],
        name="to_columns",
        compiler_params=pltpu.CompilerParams(vmem_limit_bytes=4 << 20),
    )(column, *(pltpu.with_memory_space_constraint(x, HBM) for x in (owner, source)))


def send_kernel(table, source, out, stores):
    run(
        [
            pltpu.make_async_copy(source.at[table[0, i]], out.at[table[1, i]], stores.at[i])
            for i in range(table.shape[1])
        ]
    )


def place_kernel(table, source, out):
    for i in range(table.shape[1]):
        out[table[1, i]] = source[table[0, i]]


def moved(space, table, source, pieces, name):
    kernel, scratch = place_kernel, []
    if space is HBM:
        kernel, scratch = send_kernel, [pltpu.SemaphoreType.DMA((table.shape[1],))]
    return pl.pallas_call(
        kernel,
        out_shape=space((pieces, *source.shape[1:]), source.dtype),
        in_specs=[pl.BlockSpec(memory_space=SMEM), pl.BlockSpec(memory_space=VMEM)],
        out_specs=pl.BlockSpec(memory_space=space),
        scratch_shapes=scratch,
        name=name,
        compiler_params=pltpu.CompilerParams(vmem_limit_bytes=4 << 20),
    )(table, pltpu.with_memory_space_constraint(source, VMEM))


OFFERS = ((0, 1), (-1, 0), (-1, 1), (1, 0), (1, 1), (-2, 0), (-2, 1), (2, 0), (2, 1))
REACH = (0, -1, 1, -2, 2)


def match_kernel(owned, helper, helped, *, slots):
    groups = owned.shape[0]
    ring = groups // 2
    for g in range(groups):
        helper[g] = jnp.int32(0)
        helped[g] = jnp.where(owned[g] < slots, -1, -2).astype(jnp.int32)

    def step(g, carry):
        chip = lax.div(g, jnp.int32(2))
        core = lax.rem(g, jnp.int32(2))
        need = jnp.where(owned[g] > slots, 1, 0).astype(jnp.int32)
        for chips, swap in OFFERS:
            offer = lax.rem(chip + (chips + ring), jnp.int32(ring)) * 2 + (1 - core if swap else core)
            free = jnp.where(helped[offer] == -1, 1, 0).astype(jnp.int32)

            @pl.when(need * free > 0)
            def _():
                helped[offer] = g
                helper[g] = offer

            need = need * (1 - free)
        return carry

    lax.fori_loop(jnp.int32(0), jnp.int32(groups), step, jnp.int32(0))


def matched(owned, slots):
    scalars = pl.BlockSpec(memory_space=SMEM)
    table = jax.ShapeDtypeStruct(owned.shape, jnp.int32)
    return pl.pallas_call(
        functools.partial(match_kernel, slots=slots),
        out_shape=[table, table],
        in_specs=[scalars],
        out_specs=[scalars, scalars],
        name="match",
        compiler_params=pltpu.CompilerParams(vmem_limit_bytes=1 << 20),
    )(owned)


def last_kernel(left, right, out, arrivals):
    last = left.shape[0] - 1
    run(
        [
            pltpu.make_async_copy(factor.at[last], out.at[side], arrivals.at[side])
            for side, factor in enumerate((left, right))
        ]
    )


def last_factors(left, right):
    hbm = pl.BlockSpec(memory_space=HBM)
    return pl.pallas_call(
        last_kernel,
        out_shape=VMEM((2, *left.shape[1:]), left.dtype),
        in_specs=[hbm, hbm],
        out_specs=pl.BlockSpec(memory_space=VMEM),
        scratch_shapes=[pltpu.SemaphoreType.DMA((2,))],
        name="last_factors",
        compiler_params=pltpu.CompilerParams(vmem_limit_bytes=4 << 20),
    )(*(pltpu.with_memory_space_constraint(x, HBM) for x in (left, right)))


def select_kernel(table, left, right, *rest):
    candidates, out, arrivals = rest[:-2], rest[-2], rest[-1]
    last = left.shape[0] - 1

    @pl.when(table[0] == 0)
    def _():
        run(
            [
                pltpu.make_async_copy(factor.at[last], out.at[side], arrivals.at[side])
                for side, factor in enumerate((left, right))
            ]
        )

    for index, candidate in enumerate(candidates):

        @pl.when(table[0] == index + 1)
        def _():
            run([pltpu.make_async_copy(candidate, out, arrivals.at[0])])


def selected(table, left, right, candidates):
    hbm = pl.BlockSpec(memory_space=HBM)
    operands = (left, right, *candidates)
    return pl.pallas_call(
        select_kernel,
        out_shape=VMEM(candidates[0].shape, candidates[0].dtype),
        in_specs=[pl.BlockSpec(memory_space=SMEM)] + [hbm] * len(operands),
        out_specs=pl.BlockSpec(memory_space=VMEM),
        scratch_shapes=[pltpu.SemaphoreType.DMA((2,))],
        name="select",
        compiler_params=pltpu.CompilerParams(vmem_limit_bytes=4 << 20),
    )(table, *(pltpu.with_memory_space_constraint(x, HBM) for x in operands))


def product_kernel(table, left, right, blocks, *rest):
    candidates, out, chosen, arrival = rest[:-3], rest[-3], rest[-2], rest[-1]
    size = left.shape[-1]
    slots = out.shape[1]
    last = slots - 1

    def product(k, left_matrix, right_matrix):
        block = blocks[:, k].reshape(size, size)
        half = jnp.dot(left_matrix, block, preferred_element_type=jnp.float32).astype(left.dtype)
        full = jnp.dot(half, right_matrix, preferred_element_type=jnp.float32).astype(left.dtype)
        out[:, k] = full.reshape(out.shape[0], *out.shape[2:])

    for index, candidate in enumerate(candidates):

        @pl.when(table[0] == index + 1)
        def _():
            pltpu.make_async_copy(candidate, chosen, arrival).start()

    for k in range(last):
        product(k, left[k], right[k])

    @pl.when(table[0] == 0)
    def _():
        product(last, left[last], right[last])

    @pl.when(table[0] > 0)
    def _():
        pltpu.make_async_copy(candidates[0], chosen, arrival).wait()
        product(last, chosen[0], chosen[1])


def products(table, left, right, blocks, candidates):
    slots = blocks.shape[1]
    size = left.shape[-1]
    resident = pl.BlockSpec(memory_space=VMEM)
    hbm = pl.BlockSpec(memory_space=HBM)
    return pl.pallas_call(
        product_kernel,
        out_shape=VMEM(blocks.shape, blocks.dtype),
        in_specs=[pl.BlockSpec(memory_space=SMEM)] + [resident] * 3 + [hbm] * len(candidates),
        out_specs=resident,
        scratch_shapes=[VMEM((2, size, size), left.dtype), pltpu.SemaphoreType.DMA],
        name="products",
        compiler_params=pltpu.CompilerParams(vmem_limit_bytes=16 << 20),
        cost_estimate=pl.CostEstimate(
            flops=4 * slots * size**3, transcendentals=0, bytes_accessed=4 * (left.size + blocks.size)
        ),
    )(
        table,
        *(pltpu.with_memory_space_constraint(x, VMEM) for x in (left, right, blocks)),
        *(pltpu.with_memory_space_constraint(x, HBM) for x in candidates),
    )


def shifted(array, step, size):
    return lax.ppermute(array, "grp", [(i, (i + step) % size) for i in range(size)])


def exchanged(pieces, axis):
    return lax.all_to_all(pieces, axis, split_axis=0, concat_axis=0, tiled=True)


def per_device(gradient, left_factor, right_factor, block_owner):
    local_blocks, rows, width = gradient.shape
    slots = left_factor.shape[0] - 1
    columns = lax.axis_size("fsdp")
    groups = lax.axis_size("grp")
    ring = groups // 2
    column = lax.axis_index("fsdp")
    group = lax.axis_index("grp")
    chip, core = group // 2, group % 2
    outgoing = to_columns(column.reshape(1).astype(jnp.int32), block_owner, gradient, columns, groups)
    arrived = exchanged(outgoing, "fsdp")
    mine = lax.dynamic_slice_in_dim(block_owner, column * local_blocks, local_blocks) // groups
    owners = block_owner.reshape(columns, local_blocks)
    toward = owners // groups == column
    live = jnp.any(toward, axis=1)
    target = jnp.sum(jnp.where(toward, owners % groups, 0), axis=1)
    ids = jnp.arange(columns, dtype=jnp.int32)
    earlier = (target[None, :] == target[:, None]) & live[None, :] & (ids[None, :] < ids[:, None])
    rank = jnp.sum(earlier.astype(jnp.int32), axis=1)
    members = jnp.arange(groups, dtype=jnp.int32)
    owned = jnp.sum(((target[None, :] == members[:, None]) & live[None, :]).astype(jnp.int32), axis=1)
    helper, helped = matched(owned, slots)
    target_helper = jnp.sum(jnp.where(target[:, None] == members[None, :], helper[None, :], 0), axis=1)
    slot = jnp.where(rank < slots, target * slots + rank, target_helper * slots + slots - 1)
    nth = jnp.sum((live[None, :] & (ids[None, :] < ids[:, None])).astype(jnp.int32), axis=1)
    blocks_here = jnp.arange(local_blocks, dtype=jnp.int32)
    picked = live[None, :] & (nth[None, :] == blocks_here[:, None])
    origins = jnp.sum(jnp.where(picked, ids[None, :], 0), axis=1)
    places = jnp.sum(jnp.where(picked, slot[None, :], 0), axis=1)
    own = last_factors(left_factor, right_factor)
    below = shifted(own, 2, groups)
    above = shifted(own, -2, groups)
    candidates = (below, above, shifted(below, 2, groups), shifted(above, -2, groups))
    pair = jnp.stack([group, group ^ 1])
    giver = jnp.sum(jnp.where(pair[:, None] == members[None, :], helped[None, :], 0), axis=1)
    away = (giver // 2 - chip + ring) % ring
    reach = jnp.array(REACH, dtype=jnp.int32) % ring
    index = jnp.sum(jnp.where(away[:, None] == reach[None, :], jnp.arange(len(REACH))[None, :], 0), axis=1)
    here = (giver >= 0) & (giver % 2 == core)
    passed = selected(
        jnp.where(here, index, -1)[1:].astype(jnp.int32), left_factor, right_factor, candidates
    )
    far = lax.ppermute(passed, "grp", [(i, i ^ 1) for i in range(groups)])
    source = jnp.where(giver < 0, 0, jnp.where(here, index, len(candidates) + 1))[:1].astype(jnp.int32)

    inward = jnp.stack([origins, places]).astype(jnp.int32)
    outward = jnp.stack([places, origins]).astype(jnp.int32)
    landing = jnp.stack([mine, blocks_here]).astype(jnp.int32)
    arrived, below, above, outward, landing = lax.optimization_barrier((arrived, below, above, outward, landing))
    packed = moved(HBM, inward, arrived, groups * slots, "to_slots")
    blocks = exchanged(packed.reshape(groups, slots, rows, width), "grp")
    result = products(source, left_factor, right_factor, blocks, (*candidates, far))
    returned = exchanged(result, "grp").reshape(groups * slots, rows, width)
    homeward = moved(VMEM, outward, returned, columns, "from_slots")
    home = exchanged(homeward, "fsdp")
    return moved(HBM, landing, home, local_blocks, "from_columns")


def solution(mesh):
    placed = (P("fsdp", "grp", None), P(("fsdp", "grp"), None, None), P(("fsdp", "grp"), None, None), P())
    return jax.shard_map(
        per_device, mesh=mesh, in_specs=placed, out_specs=P("fsdp", "grp", None), check_vma=False
    )
```

```python
import functools

import jax
import jax.numpy as jnp
from jax import lax
from jax.experimental import pallas as pl
from jax.experimental.pallas import tpu as pltpu
from jax.sharding import PartitionSpec as P

HBM = pltpu.HBM
VMEM = pltpu.VMEM
SMEM = pltpu.SMEM


def run(copies):
    for copy in copies:
        copy.start()
    for copy in copies:
        copy.wait()


def to_columns_kernel(column, owner, source, out, owners, pieces, loads, stores, *, groups):
    count = source.shape[0]
    owned = pltpu.make_async_copy(owner, owners, loads.at[count])
    owned.start()
    loaded = [pltpu.make_async_copy(source.at[i], pieces.at[i], loads.at[i]) for i in range(count)]
    for copy in loaded:
        copy.start()
    owned.wait()
    stored = []
    for i in range(count):
        dest = lax.div(owners[column[0] * count + i], jnp.int32(groups))
        stored.append(pltpu.make_async_copy(pieces.at[i], out.at[dest], stores.at[i]))
        loaded[i].wait()
        stored[i].start()
    for copy in stored:
        copy.wait()


def to_columns(column, owner, source, columns, groups):
    hbm = pl.BlockSpec(memory_space=HBM)
    return pl.pallas_call(
        functools.partial(to_columns_kernel, groups=groups),
        out_shape=HBM((columns, *source.shape[1:]), source.dtype),
        in_specs=[pl.BlockSpec(memory_space=SMEM), hbm, hbm],
        out_specs=hbm,
        scratch_shapes=[
            SMEM(owner.shape, owner.dtype),
            VMEM(source.shape, source.dtype),
            pltpu.SemaphoreType.DMA((source.shape[0] + 1,)),
            pltpu.SemaphoreType.DMA((source.shape[0],)),
        ],
        name="to_columns",
        compiler_params=pltpu.CompilerParams(vmem_limit_bytes=4 << 20),
    )(column, *(pltpu.with_memory_space_constraint(x, HBM) for x in (owner, source)))


def send_kernel(table, source, out, stores):
    run(
        [
            pltpu.make_async_copy(source.at[table[0, i]], out.at[table[1, i]], stores.at[i])
            for i in range(table.shape[1])
        ]
    )


def place_kernel(table, source, out):
    for i in range(table.shape[1]):
        out[table[1, i]] = source[table[0, i]]


def moved(space, table, source, pieces, name):
    kernel, scratch = place_kernel, []
    if space is HBM:
        kernel, scratch = send_kernel, [pltpu.SemaphoreType.DMA((table.shape[1],))]
    return pl.pallas_call(
        kernel,
        out_shape=space((pieces, *source.shape[1:]), source.dtype),
        in_specs=[pl.BlockSpec(memory_space=SMEM), pl.BlockSpec(memory_space=VMEM)],
        out_specs=pl.BlockSpec(memory_space=space),
        scratch_shapes=scratch,
        name=name,
        compiler_params=pltpu.CompilerParams(vmem_limit_bytes=4 << 20),
    )(table, pltpu.with_memory_space_constraint(source, VMEM))


OFFERS = ((0, 1), (-1, 0), (-1, 1), (1, 0), (1, 1), (-2, 0), (-2, 1), (2, 0), (2, 1))
REACH = (0, -1, 1, -2, 2)


def match_kernel(owned, helper, helped, *, slots):
    groups = owned.shape[0]
    ring = groups // 2
    for g in range(groups):
        helper[g] = jnp.int32(0)
        helped[g] = jnp.where(owned[g] < slots, -1, -2).astype(jnp.int32)

    def step(g, carry):
        chip = lax.div(g, jnp.int32(2))
        core = lax.rem(g, jnp.int32(2))
        need = jnp.where(owned[g] > slots, 1, 0).astype(jnp.int32)
        for chips, swap in OFFERS:
            offer = lax.rem(chip + (chips + ring), jnp.int32(ring)) * 2 + (1 - core if swap else core)
            free = jnp.where(helped[offer] == -1, 1, 0).astype(jnp.int32)

            @pl.when(need * free > 0)
            def _():
                helped[offer] = g
                helper[g] = offer

            need = need * (1 - free)
        return carry

    lax.fori_loop(jnp.int32(0), jnp.int32(groups), step, jnp.int32(0))


def matched(owned, slots):
    scalars = pl.BlockSpec(memory_space=SMEM)
    table = jax.ShapeDtypeStruct(owned.shape, jnp.int32)
    return pl.pallas_call(
        functools.partial(match_kernel, slots=slots),
        out_shape=[table, table],
        in_specs=[scalars],
        out_specs=[scalars, scalars],
        name="match",
        compiler_params=pltpu.CompilerParams(vmem_limit_bytes=1 << 20),
    )(owned)


def last_kernel(left, right, out, arrivals):
    last = left.shape[0] - 1
    run(
        [
            pltpu.make_async_copy(factor.at[last], out.at[side], arrivals.at[side])
            for side, factor in enumerate((left, right))
        ]
    )


def last_factors(left, right):
    hbm = pl.BlockSpec(memory_space=HBM)
    return pl.pallas_call(
        last_kernel,
        out_shape=VMEM((2, *left.shape[1:]), left.dtype),
        in_specs=[hbm, hbm],
        out_specs=pl.BlockSpec(memory_space=VMEM),
        scratch_shapes=[pltpu.SemaphoreType.DMA((2,))],
        name="last_factors",
        compiler_params=pltpu.CompilerParams(vmem_limit_bytes=4 << 20),
    )(*(pltpu.with_memory_space_constraint(x, HBM) for x in (left, right)))


def select_kernel(table, left, right, *rest):
    candidates, out, arrivals = rest[:-2], rest[-2], rest[-1]
    last = left.shape[0] - 1

    @pl.when(table[0] == 0)
    def _():
        run(
            [
                pltpu.make_async_copy(factor.at[last], out.at[side], arrivals.at[side])
                for side, factor in enumerate((left, right))
            ]
        )

    for index, candidate in enumerate(candidates):

        @pl.when(table[0] == index + 1)
        def _():
            run([pltpu.make_async_copy(candidate, out, arrivals.at[0])])


def selected(table, left, right, candidates):
    hbm = pl.BlockSpec(memory_space=HBM)
    operands = (left, right, *candidates)
    return pl.pallas_call(
        select_kernel,
        out_shape=VMEM(candidates[0].shape, candidates[0].dtype),
        in_specs=[pl.BlockSpec(memory_space=SMEM)] + [hbm] * len(operands),
        out_specs=pl.BlockSpec(memory_space=VMEM),
        scratch_shapes=[pltpu.SemaphoreType.DMA((2,))],
        name="select",
        compiler_params=pltpu.CompilerParams(vmem_limit_bytes=4 << 20),
    )(table, *(pltpu.with_memory_space_constraint(x, HBM) for x in operands))


def choose_kernel(table, left, right, *rest):
    candidates, chosen, arrivals = rest[:-2], rest[-2], rest[-1]
    last = chosen.shape[0] - 1
    sides = tuple(enumerate((left, right)))

    def own(k):
        return [pltpu.make_async_copy(factor.at[k], chosen.at[k, side], arrivals.at[k, side]) for side, factor in sides]

    ahead = [copy for k in range(last) for copy in own(k)]
    for copy in ahead:
        copy.start()

    @pl.when(table[0] == 0)
    def _():
        run(own(last))

    for index, candidate in enumerate(candidates):

        @pl.when(table[0] == index + 1)
        def _():
            run([pltpu.make_async_copy(candidate, chosen.at[last], arrivals.at[last, 0])])

    for copy in ahead:
        copy.wait()


def chosen_factors(table, slots, left, right, candidates):
    hbm = pl.BlockSpec(memory_space=HBM)
    operands = (left, right, *candidates)
    return pl.pallas_call(
        choose_kernel,
        out_shape=VMEM((slots, 2, *left.shape[1:]), left.dtype),
        in_specs=[pl.BlockSpec(memory_space=SMEM)] + [hbm] * len(operands),
        out_specs=pl.BlockSpec(memory_space=VMEM),
        scratch_shapes=[pltpu.SemaphoreType.DMA((slots, 2))],
        name="choose",
        compiler_params=pltpu.CompilerParams(vmem_limit_bytes=4 << 20),
    )(table, *(pltpu.with_memory_space_constraint(x, HBM) for x in operands))


def product_kernel(factors, blocks, out):
    size = factors.shape[-1]
    for k in range(out.shape[1]):
        block = blocks[:, k].reshape(size, size)
        half = jnp.dot(factors[k, 0], block, preferred_element_type=jnp.float32).astype(blocks.dtype)
        full = jnp.dot(half, factors[k, 1], preferred_element_type=jnp.float32).astype(blocks.dtype)
        out[:, k] = full.reshape(out.shape[0], *out.shape[2:])


def products(factors, blocks):
    resident = pl.BlockSpec(memory_space=VMEM)
    return pl.pallas_call(
        product_kernel,
        out_shape=VMEM(blocks.shape, blocks.dtype),
        in_specs=[resident, resident],
        out_specs=resident,
        name="products",
        compiler_params=pltpu.CompilerParams(vmem_limit_bytes=16 << 20),
        cost_estimate=pl.CostEstimate(
            flops=2 * factors.size * factors.shape[-1], transcendentals=0, bytes_accessed=4 * (factors.size + blocks.size)
        ),
    )(*(pltpu.with_memory_space_constraint(x, VMEM) for x in (factors, blocks)))


def shifted(array, step, size):
    return lax.ppermute(array, "grp", [(i, (i + step) % size) for i in range(size)])


def exchanged(pieces, axis):
    return lax.all_to_all(pieces, axis, split_axis=0, concat_axis=0, tiled=True)


def per_device(gradient, left_factor, right_factor, block_owner):
    local_blocks, rows, width = gradient.shape
    slots = left_factor.shape[0] - 1
    columns = lax.axis_size("fsdp")
    groups = lax.axis_size("grp")
    ring = groups // 2
    column = lax.axis_index("fsdp")
    group = lax.axis_index("grp")
    chip, core = group // 2, group % 2
    outgoing = to_columns(column.reshape(1).astype(jnp.int32), block_owner, gradient, columns, groups)
    arrived = exchanged(outgoing, "fsdp")
    mine = lax.dynamic_slice_in_dim(block_owner, column * local_blocks, local_blocks) // groups
    owners = block_owner.reshape(columns, local_blocks)
    toward = owners // groups == column
    live = jnp.any(toward, axis=1)
    target = jnp.sum(jnp.where(toward, owners % groups, 0), axis=1)
    ids = jnp.arange(columns, dtype=jnp.int32)
    earlier = (target[None, :] == target[:, None]) & live[None, :] & (ids[None, :] < ids[:, None])
    rank = jnp.sum(earlier.astype(jnp.int32), axis=1)
    members = jnp.arange(groups, dtype=jnp.int32)
    owned = jnp.sum(((target[None, :] == members[:, None]) & live[None, :]).astype(jnp.int32), axis=1)
    helper, helped = matched(owned, slots)
    target_helper = jnp.sum(jnp.where(target[:, None] == members[None, :], helper[None, :], 0), axis=1)
    slot = jnp.where(rank < slots, target * slots + rank, target_helper * slots + slots - 1)
    nth = jnp.sum((live[None, :] & (ids[None, :] < ids[:, None])).astype(jnp.int32), axis=1)
    blocks_here = jnp.arange(local_blocks, dtype=jnp.int32)
    picked = live[None, :] & (nth[None, :] == blocks_here[:, None])
    origins = jnp.sum(jnp.where(picked, ids[None, :], 0), axis=1)
    places = jnp.sum(jnp.where(picked, slot[None, :], 0), axis=1)
    own = last_factors(left_factor, right_factor)
    below = shifted(own, 2, groups)
    above = shifted(own, -2, groups)
    candidates = (below, above, shifted(below, 2, groups), shifted(above, -2, groups))
    pair = jnp.stack([group, group ^ 1])
    giver = jnp.sum(jnp.where(pair[:, None] == members[None, :], helped[None, :], 0), axis=1)
    away = (giver // 2 - chip + ring) % ring
    reach = jnp.array(REACH, dtype=jnp.int32) % ring
    index = jnp.sum(jnp.where(away[:, None] == reach[None, :], jnp.arange(len(REACH))[None, :], 0), axis=1)
    here = (giver >= 0) & (giver % 2 == core)
    passed = selected(
        jnp.where(here, index, -1)[1:].astype(jnp.int32), left_factor, right_factor, candidates
    )
    far = lax.ppermute(passed, "grp", [(i, i ^ 1) for i in range(groups)])
    source = jnp.where(giver < 0, 0, jnp.where(here, index, len(candidates) + 1))[:1].astype(jnp.int32)

    inward = jnp.stack([origins, places]).astype(jnp.int32)
    outward = jnp.stack([places, origins]).astype(jnp.int32)
    landing = jnp.stack([mine, blocks_here]).astype(jnp.int32)
    arrived, below, above, outward, landing = lax.optimization_barrier((arrived, below, above, outward, landing))
    packed = moved(HBM, inward, arrived, groups * slots, "to_slots")
    factors = chosen_factors(source, slots, left_factor, right_factor, (*candidates, far))
    blocks = exchanged(packed.reshape(groups, slots, rows, width), "grp")
    result = products(factors, blocks)
    returned = exchanged(result, "grp").reshape(groups * slots, rows, width)
    homeward = moved(VMEM, outward, returned, columns, "from_slots")
    home = exchanged(homeward, "fsdp")
    return moved(HBM, landing, home, local_blocks, "from_columns")


def solution(mesh):
    placed = (P("fsdp", "grp", None), P(("fsdp", "grp"), None, None), P(("fsdp", "grp"), None, None), P())
    return jax.shard_map(
        per_device, mesh=mesh, in_specs=placed, out_specs=P("fsdp", "grp", None), check_vma=False
    )
```

```python
import functools

import jax
import jax.numpy as jnp
from jax import lax
from jax.experimental import pallas as pl
from jax.experimental.pallas import tpu as pltpu
from jax.sharding import PartitionSpec as P

HBM = pltpu.HBM
VMEM = pltpu.VMEM
SMEM = pltpu.SMEM


def run(copies):
    for copy in copies:
        copy.start()
    for copy in copies:
        copy.wait()


def to_columns_kernel(
    column, owner, source, left, right, out, factors, owners, pieces, loads, stores, arrivals, *, groups
):
    count = source.shape[0]
    owned = pltpu.make_async_copy(owner, owners, loads.at[count])
    owned.start()
    loaded = [pltpu.make_async_copy(source.at[i], pieces.at[i], loads.at[i]) for i in range(count)]
    for copy in loaded:
        copy.start()
    last = left.shape[0] - 1
    fetched = [
        pltpu.make_async_copy(factor.at[last], factors.at[side], arrivals.at[side])
        for side, factor in enumerate((left, right))
    ]
    for copy in fetched:
        copy.start()
    owned.wait()
    stored = []
    for i in range(count):
        dest = lax.div(owners[column[0] * count + i], jnp.int32(groups))
        stored.append(pltpu.make_async_copy(pieces.at[i], out.at[dest], stores.at[i]))
        loaded[i].wait()
        stored[i].start()
    for copy in stored + fetched:
        copy.wait()


def to_columns(column, owner, source, left, right, columns, groups):
    hbm = pl.BlockSpec(memory_space=HBM)
    return pl.pallas_call(
        functools.partial(to_columns_kernel, groups=groups),
        out_shape=[HBM((columns, *source.shape[1:]), source.dtype), VMEM((2, *left.shape[1:]), left.dtype)],
        in_specs=[pl.BlockSpec(memory_space=SMEM)] + [hbm] * 4,
        out_specs=[hbm, pl.BlockSpec(memory_space=VMEM)],
        scratch_shapes=[
            SMEM(owner.shape, owner.dtype),
            VMEM(source.shape, source.dtype),
            pltpu.SemaphoreType.DMA((source.shape[0] + 1,)),
            pltpu.SemaphoreType.DMA((source.shape[0],)),
            pltpu.SemaphoreType.DMA((2,)),
        ],
        name="to_columns",
        compiler_params=pltpu.CompilerParams(vmem_limit_bytes=4 << 20),
    )(column, *(pltpu.with_memory_space_constraint(x, HBM) for x in (owner, source, left, right)))


def send_kernel(table, source, out, stores):
    run(
        [
            pltpu.make_async_copy(source.at[table[0, i]], out.at[table[1, i]], stores.at[i])
            for i in range(table.shape[1])
        ]
    )


def place_kernel(table, source, out):
    for i in range(table.shape[1]):
        out[table[1, i]] = source[table[0, i]]


def moved(space, table, source, pieces, name):
    kernel, scratch = place_kernel, []
    if space is HBM:
        kernel, scratch = send_kernel, [pltpu.SemaphoreType.DMA((table.shape[1],))]
    return pl.pallas_call(
        kernel,
        out_shape=space((pieces, *source.shape[1:]), source.dtype),
        in_specs=[pl.BlockSpec(memory_space=SMEM), pl.BlockSpec(memory_space=VMEM)],
        out_specs=pl.BlockSpec(memory_space=space),
        scratch_shapes=scratch,
        name=name,
        compiler_params=pltpu.CompilerParams(vmem_limit_bytes=4 << 20),
    )(table, pltpu.with_memory_space_constraint(source, VMEM))


OFFERS = ((0, 1), (-1, 0), (-1, 1), (1, 0), (1, 1), (-2, 0), (-2, 1), (2, 0), (2, 1))
REACH = (0, -1, 1, -2, 2)


def match_kernel(owned, helper, helped, *, slots):
    groups = owned.shape[0]
    ring = groups // 2
    for g in range(groups):
        helper[g] = jnp.int32(0)
        helped[g] = jnp.where(owned[g] < slots, -1, -2).astype(jnp.int32)

    def step(g, carry):
        chip = lax.div(g, jnp.int32(2))
        core = lax.rem(g, jnp.int32(2))
        need = jnp.where(owned[g] > slots, 1, 0).astype(jnp.int32)
        for chips, swap in OFFERS:
            offer = lax.rem(chip + (chips + ring), jnp.int32(ring)) * 2 + (1 - core if swap else core)
            free = jnp.where(helped[offer] == -1, 1, 0).astype(jnp.int32)

            @pl.when(need * free > 0)
            def _():
                helped[offer] = g
                helper[g] = offer

            need = need * (1 - free)
        return carry

    lax.fori_loop(jnp.int32(0), jnp.int32(groups), step, jnp.int32(0))


def matched(owned, slots):
    scalars = pl.BlockSpec(memory_space=SMEM)
    table = jax.ShapeDtypeStruct(owned.shape, jnp.int32)
    return pl.pallas_call(
        functools.partial(match_kernel, slots=slots),
        out_shape=[table, table],
        in_specs=[scalars],
        out_specs=[scalars, scalars],
        name="match",
        compiler_params=pltpu.CompilerParams(vmem_limit_bytes=1 << 20),
    )(owned)


def select_kernel(table, left, right, *rest):
    candidates, out, arrivals = rest[:-2], rest[-2], rest[-1]
    last = left.shape[0] - 1

    @pl.when(table[0] == 0)
    def _():
        run(
            [
                pltpu.make_async_copy(factor.at[last], out.at[side], arrivals.at[side])
                for side, factor in enumerate((left, right))
            ]
        )

    for index, candidate in enumerate(candidates):

        @pl.when(table[0] == index + 1)
        def _():
            run([pltpu.make_async_copy(candidate, out, arrivals.at[0])])


def selected(table, left, right, candidates):
    hbm = pl.BlockSpec(memory_space=HBM)
    operands = (left, right, *candidates)
    return pl.pallas_call(
        select_kernel,
        out_shape=VMEM(candidates[0].shape, candidates[0].dtype),
        in_specs=[pl.BlockSpec(memory_space=SMEM)] + [hbm] * len(operands),
        out_specs=pl.BlockSpec(memory_space=VMEM),
        scratch_shapes=[pltpu.SemaphoreType.DMA((2,))],
        name="select",
        compiler_params=pltpu.CompilerParams(vmem_limit_bytes=4 << 20),
    )(table, *(pltpu.with_memory_space_constraint(x, HBM) for x in operands))


def choose_kernel(table, left, right, *rest):
    candidates, chosen, arrivals = rest[:-2], rest[-2], rest[-1]
    last = chosen.shape[0] - 1
    sides = tuple(enumerate((left, right)))

    def own(k):
        return [pltpu.make_async_copy(factor.at[k], chosen.at[k, side], arrivals.at[k, side]) for side, factor in sides]

    ahead = [copy for k in range(last) for copy in own(k)]
    for copy in ahead:
        copy.start()

    @pl.when(table[0] == 0)
    def _():
        run(own(last))

    for index, candidate in enumerate(candidates):

        @pl.when(table[0] == index + 1)
        def _():
            run([pltpu.make_async_copy(candidate, chosen.at[last], arrivals.at[last, 0])])

    for copy in ahead:
        copy.wait()


def chosen_factors(table, slots, left, right, candidates):
    hbm = pl.BlockSpec(memory_space=HBM)
    operands = (left, right, *candidates)
    return pl.pallas_call(
        choose_kernel,
        out_shape=VMEM((slots, 2, *left.shape[1:]), left.dtype),
        in_specs=[pl.BlockSpec(memory_space=SMEM)] + [hbm] * len(operands),
        out_specs=pl.BlockSpec(memory_space=VMEM),
        scratch_shapes=[pltpu.SemaphoreType.DMA((slots, 2))],
        name="choose",
        compiler_params=pltpu.CompilerParams(vmem_limit_bytes=4 << 20),
    )(table, *(pltpu.with_memory_space_constraint(x, HBM) for x in operands))


def product_kernel(factors, blocks, out):
    size = factors.shape[-1]
    for k in range(out.shape[1]):
        block = blocks[:, k].reshape(size, size)
        half = jnp.dot(factors[k, 0], block, preferred_element_type=jnp.float32).astype(blocks.dtype)
        full = jnp.dot(half, factors[k, 1], preferred_element_type=jnp.float32).astype(blocks.dtype)
        out[:, k] = full.reshape(out.shape[0], *out.shape[2:])


def products(factors, blocks):
    resident = pl.BlockSpec(memory_space=VMEM)
    return pl.pallas_call(
        product_kernel,
        out_shape=VMEM(blocks.shape, blocks.dtype),
        in_specs=[resident, resident],
        out_specs=resident,
        name="products",
        compiler_params=pltpu.CompilerParams(vmem_limit_bytes=16 << 20),
        cost_estimate=pl.CostEstimate(
            flops=2 * factors.size * factors.shape[-1], transcendentals=0, bytes_accessed=4 * (factors.size + blocks.size)
        ),
    )(*(pltpu.with_memory_space_constraint(x, VMEM) for x in (factors, blocks)))


def shifted(array, step, size):
    return lax.ppermute(array, "grp", [(i, (i + step) % size) for i in range(size)])


def exchanged(pieces, axis):
    return lax.all_to_all(pieces, axis, split_axis=0, concat_axis=0, tiled=True)


def per_device(gradient, left_factor, right_factor, block_owner):
    local_blocks, rows, width = gradient.shape
    slots = left_factor.shape[0] - 1
    columns = lax.axis_size("fsdp")
    groups = lax.axis_size("grp")
    ring = groups // 2
    column = lax.axis_index("fsdp")
    group = lax.axis_index("grp")
    chip, core = group // 2, group % 2
    outgoing, own = to_columns(
        column.reshape(1).astype(jnp.int32), block_owner, gradient, left_factor, right_factor, columns, groups
    )
    arrived = exchanged(outgoing, "fsdp")
    mine = lax.dynamic_slice_in_dim(block_owner, column * local_blocks, local_blocks) // groups
    owners = block_owner.reshape(columns, local_blocks)
    toward = owners // groups == column
    live = jnp.any(toward, axis=1)
    target = jnp.sum(jnp.where(toward, owners % groups, 0), axis=1)
    ids = jnp.arange(columns, dtype=jnp.int32)
    earlier = (target[None, :] == target[:, None]) & live[None, :] & (ids[None, :] < ids[:, None])
    rank = jnp.sum(earlier.astype(jnp.int32), axis=1)
    members = jnp.arange(groups, dtype=jnp.int32)
    owned = jnp.sum(((target[None, :] == members[:, None]) & live[None, :]).astype(jnp.int32), axis=1)
    helper, helped = matched(owned, slots)
    target_helper = jnp.sum(jnp.where(target[:, None] == members[None, :], helper[None, :], 0), axis=1)
    slot = jnp.where(rank < slots, target * slots + rank, target_helper * slots + slots - 1)
    nth = jnp.sum((live[None, :] & (ids[None, :] < ids[:, None])).astype(jnp.int32), axis=1)
    blocks_here = jnp.arange(local_blocks, dtype=jnp.int32)
    picked = live[None, :] & (nth[None, :] == blocks_here[:, None])
    origins = jnp.sum(jnp.where(picked, ids[None, :], 0), axis=1)
    places = jnp.sum(jnp.where(picked, slot[None, :], 0), axis=1)
    below = shifted(own, 2, groups)
    above = shifted(own, -2, groups)
    candidates = (below, above, shifted(below, 2, groups), shifted(above, -2, groups))
    pair = jnp.stack([group, group ^ 1])
    giver = jnp.sum(jnp.where(pair[:, None] == members[None, :], helped[None, :], 0), axis=1)
    away = (giver // 2 - chip + ring) % ring
    reach = jnp.array(REACH, dtype=jnp.int32) % ring
    index = jnp.sum(jnp.where(away[:, None] == reach[None, :], jnp.arange(len(REACH))[None, :], 0), axis=1)
    here = (giver >= 0) & (giver % 2 == core)
    passed = selected(
        jnp.where(here, index, -1)[1:].astype(jnp.int32), left_factor, right_factor, candidates
    )
    far = lax.ppermute(passed, "grp", [(i, i ^ 1) for i in range(groups)])
    source = jnp.where(giver < 0, 0, jnp.where(here, index, len(candidates) + 1))[:1].astype(jnp.int32)

    inward = jnp.stack([origins, places]).astype(jnp.int32)
    outward = jnp.stack([places, origins]).astype(jnp.int32)
    landing = jnp.stack([mine, blocks_here]).astype(jnp.int32)
    arrived, below, above, outward, landing = lax.optimization_barrier((arrived, below, above, outward, landing))
    packed = moved(HBM, inward, arrived, groups * slots, "to_slots")
    factors = chosen_factors(source, slots, left_factor, right_factor, (*candidates, far))
    blocks = exchanged(packed.reshape(groups, slots, rows, width), "grp")
    result = products(factors, blocks)
    returned = exchanged(result, "grp").reshape(groups * slots, rows, width)
    homeward = moved(VMEM, outward, returned, columns, "from_slots")
    home = exchanged(homeward, "fsdp")
    return moved(HBM, landing, home, local_blocks, "from_columns")


def solution(mesh):
    placed = (P("fsdp", "grp", None), P(("fsdp", "grp"), None, None), P(("fsdp", "grp"), None, None), P())
    return jax.shard_map(
        per_device, mesh=mesh, in_specs=placed, out_specs=P("fsdp", "grp", None), check_vma=False
    )
```

```python
import functools

import jax
import jax.numpy as jnp
from jax import lax
from jax.experimental import pallas as pl
from jax.experimental.pallas import tpu as pltpu
from jax.sharding import PartitionSpec as P

HBM = pltpu.HBM
VMEM = pltpu.VMEM
SMEM = pltpu.SMEM


def run(copies):
    for copy in copies:
        copy.start()
    for copy in copies:
        copy.wait()


def to_columns_kernel(
    column, owner, source, left, right, out, factors, owners, pieces, loads, stores, arrivals, *, groups
):
    count = source.shape[0]
    owned = pltpu.make_async_copy(owner, owners, loads.at[count])
    owned.start()
    loaded = [pltpu.make_async_copy(source.at[i], pieces.at[i], loads.at[i]) for i in range(count)]
    for copy in loaded:
        copy.start()
    last = left.shape[0] - 1
    fetched = [
        pltpu.make_async_copy(factor.at[last], factors.at[side], arrivals.at[side])
        for side, factor in enumerate((left, right))
    ]
    for copy in fetched:
        copy.start()
    owned.wait()
    stored = []
    for i in range(count):
        dest = lax.div(owners[column[0] * count + i], jnp.int32(groups))
        stored.append(pltpu.make_async_copy(pieces.at[i], out.at[dest], stores.at[i]))
        loaded[i].wait()
        stored[i].start()
    for copy in stored + fetched:
        copy.wait()


def to_columns(column, owner, source, left, right, columns, groups):
    hbm = pl.BlockSpec(memory_space=HBM)
    return pl.pallas_call(
        functools.partial(to_columns_kernel, groups=groups),
        out_shape=[HBM((columns, *source.shape[1:]), source.dtype), VMEM((2, *left.shape[1:]), left.dtype)],
        in_specs=[pl.BlockSpec(memory_space=SMEM)] + [hbm] * 4,
        out_specs=[hbm, pl.BlockSpec(memory_space=VMEM)],
        scratch_shapes=[
            SMEM(owner.shape, owner.dtype),
            VMEM(source.shape, source.dtype),
            pltpu.SemaphoreType.DMA((source.shape[0] + 1,)),
            pltpu.SemaphoreType.DMA((source.shape[0],)),
            pltpu.SemaphoreType.DMA((2,)),
        ],
        name="to_columns",
        compiler_params=pltpu.CompilerParams(vmem_limit_bytes=4 << 20),
    )(column, *(pltpu.with_memory_space_constraint(x, HBM) for x in (owner, source, left, right)))


def send_kernel(table, source, out, stores):
    run(
        [
            pltpu.make_async_copy(source.at[table[0, i]], out.at[table[1, i]], stores.at[i])
            for i in range(table.shape[1])
        ]
    )


def place_kernel(table, source, out):
    for i in range(table.shape[1]):
        out[table[1, i]] = source[table[0, i]]


def moved(space, table, source, pieces, name):
    kernel, scratch = place_kernel, []
    if space is HBM:
        kernel, scratch = send_kernel, [pltpu.SemaphoreType.DMA((table.shape[1],))]
    return pl.pallas_call(
        kernel,
        out_shape=space((pieces, *source.shape[1:]), source.dtype),
        in_specs=[pl.BlockSpec(memory_space=SMEM), pl.BlockSpec(memory_space=VMEM)],
        out_specs=pl.BlockSpec(memory_space=space),
        scratch_shapes=scratch,
        name=name,
        compiler_params=pltpu.CompilerParams(vmem_limit_bytes=4 << 20),
    )(table, pltpu.with_memory_space_constraint(source, VMEM))


OFFERS = ((0, 1), (-1, 0), (-1, 1), (1, 0), (1, 1), (-2, 0), (-2, 1), (2, 0), (2, 1))
REACH = (0, -1, 1, -2, 2)


def match_kernel(owned, helper, helped, *, slots):
    groups = owned.shape[0]
    ring = groups // 2
    for g in range(groups):
        helper[g] = jnp.int32(0)
        helped[g] = jnp.where(owned[g] < slots, -1, -2).astype(jnp.int32)

    def step(g, carry):
        chip = lax.div(g, jnp.int32(2))
        core = lax.rem(g, jnp.int32(2))
        need = jnp.where(owned[g] > slots, 1, 0).astype(jnp.int32)
        for chips, swap in OFFERS:
            offer = lax.rem(chip + (chips + ring), jnp.int32(ring)) * 2 + (1 - core if swap else core)
            free = jnp.where(helped[offer] == -1, 1, 0).astype(jnp.int32)

            @pl.when(need * free > 0)
            def _():
                helped[offer] = g
                helper[g] = offer

            need = need * (1 - free)
        return carry

    lax.fori_loop(jnp.int32(0), jnp.int32(groups), step, jnp.int32(0))


def matched(owned, slots):
    scalars = pl.BlockSpec(memory_space=SMEM)
    table = jax.ShapeDtypeStruct(owned.shape, jnp.int32)
    return pl.pallas_call(
        functools.partial(match_kernel, slots=slots),
        out_shape=[table, table],
        in_specs=[scalars],
        out_specs=[scalars, scalars],
        name="match",
        compiler_params=pltpu.CompilerParams(vmem_limit_bytes=1 << 20),
    )(owned)


def select_kernel(table, left, right, *rest):
    candidates, out, arrivals = rest[:-2], rest[-2], rest[-1]
    last = left.shape[0] - 1

    @pl.when(table[0] == 0)
    def _():
        run(
            [
                pltpu.make_async_copy(factor.at[last], out.at[side], arrivals.at[side])
                for side, factor in enumerate((left, right))
            ]
        )

    for index, candidate in enumerate(candidates):

        @pl.when(table[0] == index + 1)
        def _():
            run([pltpu.make_async_copy(candidate, out, arrivals.at[0])])


def selected(table, left, right, candidates):
    hbm = pl.BlockSpec(memory_space=HBM)
    operands = (left, right, *candidates)
    return pl.pallas_call(
        select_kernel,
        out_shape=VMEM(candidates[0].shape, candidates[0].dtype),
        in_specs=[pl.BlockSpec(memory_space=SMEM)] + [hbm] * len(operands),
        out_specs=pl.BlockSpec(memory_space=VMEM),
        scratch_shapes=[pltpu.SemaphoreType.DMA((2,))],
        name="select",
        compiler_params=pltpu.CompilerParams(vmem_limit_bytes=4 << 20),
    )(table, *(pltpu.with_memory_space_constraint(x, HBM) for x in operands))


def choose_kernel(table, left, right, *rest):
    candidates, chosen, arrivals = rest[:-2], rest[-2], rest[-1]
    last = chosen.shape[0] - 1
    sides = tuple(enumerate((left, right)))

    def own(k):
        return [pltpu.make_async_copy(factor.at[k], chosen.at[k, side], arrivals.at[k, side]) for side, factor in sides]

    ahead = [copy for k in range(last) for copy in own(k)]
    for copy in ahead:
        copy.start()

    @pl.when(table[0] == 0)
    def _():
        run(own(last))

    for index, candidate in enumerate(candidates):

        @pl.when(table[0] == index + 1)
        def _():
            run([pltpu.make_async_copy(candidate, chosen.at[last], arrivals.at[last, 0])])

    for copy in ahead:
        copy.wait()


def chosen_factors(table, slots, left, right, candidates):
    hbm = pl.BlockSpec(memory_space=HBM)
    operands = (left, right, *candidates)
    return pl.pallas_call(
        choose_kernel,
        out_shape=VMEM((slots, 2, *left.shape[1:]), left.dtype),
        in_specs=[pl.BlockSpec(memory_space=SMEM)] + [hbm] * len(operands),
        out_specs=pl.BlockSpec(memory_space=VMEM),
        scratch_shapes=[pltpu.SemaphoreType.DMA((slots, 2))],
        name="choose",
        compiler_params=pltpu.CompilerParams(vmem_limit_bytes=4 << 20),
    )(table, *(pltpu.with_memory_space_constraint(x, HBM) for x in operands))


def product_kernel(factors, blocks, out):
    size = factors.shape[-1]
    for k in range(out.shape[1]):
        block = blocks[:, k].reshape(size, size)
        half = jnp.dot(factors[k, 0], block, preferred_element_type=jnp.float32).astype(blocks.dtype)
        full = jnp.dot(half, factors[k, 1], preferred_element_type=jnp.float32).astype(blocks.dtype)
        out[:, k] = full.reshape(out.shape[0], *out.shape[2:])


def products(factors, blocks):
    resident = pl.BlockSpec(memory_space=VMEM)
    return pl.pallas_call(
        product_kernel,
        out_shape=VMEM(blocks.shape, blocks.dtype),
        in_specs=[resident, resident],
        out_specs=resident,
        name="products",
        compiler_params=pltpu.CompilerParams(vmem_limit_bytes=16 << 20),
        cost_estimate=pl.CostEstimate(
            flops=2 * factors.size * factors.shape[-1], transcendentals=0, bytes_accessed=4 * (factors.size + blocks.size)
        ),
    )(*(pltpu.with_memory_space_constraint(x, VMEM) for x in (factors, blocks)))


def shifted(array, step, size):
    return lax.ppermute(array, "grp", [(i, (i + step) % size) for i in range(size)])


def exchanged(pieces, axis):
    return lax.all_to_all(pieces, axis, split_axis=0, concat_axis=0, tiled=True)


def per_device(gradient, left_factor, right_factor, block_owner):
    local_blocks, rows, width = gradient.shape
    slots = left_factor.shape[0] - 1
    columns = lax.axis_size("fsdp")
    groups = lax.axis_size("grp")
    ring = groups // 2
    column = lax.axis_index("fsdp")
    group = lax.axis_index("grp")
    chip, core = group // 2, group % 2
    outgoing, own = to_columns(
        column.reshape(1).astype(jnp.int32), block_owner, gradient, left_factor, right_factor, columns, groups
    )
    arrived = exchanged(outgoing, "fsdp")
    mine = lax.dynamic_slice_in_dim(block_owner, column * local_blocks, local_blocks) // groups
    owners = block_owner.reshape(columns, local_blocks)
    toward = owners // groups == column
    live = jnp.any(toward, axis=1)
    target = jnp.sum(jnp.where(toward, owners % groups, 0), axis=1)
    ids = jnp.arange(columns, dtype=jnp.int32)
    earlier = (target[None, :] == target[:, None]) & live[None, :] & (ids[None, :] < ids[:, None])
    rank = jnp.sum(earlier.astype(jnp.int32), axis=1)
    members = jnp.arange(groups, dtype=jnp.int32)
    owned = jnp.sum(((target[None, :] == members[:, None]) & live[None, :]).astype(jnp.int32), axis=1)
    helper, helped = matched(owned, slots)
    target_helper = jnp.sum(jnp.where(target[:, None] == members[None, :], helper[None, :], 0), axis=1)
    slot = jnp.where(rank < slots, target * slots + rank, target_helper * slots + slots - 1)
    nth = jnp.sum((live[None, :] & (ids[None, :] < ids[:, None])).astype(jnp.int32), axis=1)
    blocks_here = jnp.arange(local_blocks, dtype=jnp.int32)
    picked = live[None, :] & (nth[None, :] == blocks_here[:, None])
    origins = jnp.sum(jnp.where(picked, ids[None, :], 0), axis=1)
    places = jnp.sum(jnp.where(picked, slot[None, :], 0), axis=1)
    below = shifted(own, 2, groups)
    above = shifted(own, -2, groups)
    candidates = (below, above, shifted(below, 2, groups), shifted(above, -2, groups))
    pair = jnp.stack([group, group ^ 1])
    giver = jnp.sum(jnp.where(pair[:, None] == members[None, :], helped[None, :], 0), axis=1)
    away = (giver // 2 - chip + ring) % ring
    reach = jnp.array(REACH, dtype=jnp.int32) % ring
    index = jnp.sum(jnp.where(away[:, None] == reach[None, :], jnp.arange(len(REACH))[None, :], 0), axis=1)
    here = (giver >= 0) & (giver % 2 == core)
    passed = selected(
        jnp.where(here, index, -1)[1:].astype(jnp.int32), left_factor, right_factor, candidates
    )
    far = lax.ppermute(passed, "grp", [(i, i ^ 1) for i in range(groups)])
    source = jnp.where(giver < 0, 0, jnp.where(here, index, len(candidates) + 1))[:1].astype(jnp.int32)

    inward = jnp.stack([origins, places]).astype(jnp.int32)
    outward = jnp.stack([places, origins]).astype(jnp.int32)
    landing = jnp.stack([mine, blocks_here]).astype(jnp.int32)
    arrived, below, above, outward, landing = lax.optimization_barrier((arrived, below, above, outward, landing))
    packed = moved(HBM, inward, arrived, groups * slots, "to_slots")
    factors = chosen_factors(source, slots, left_factor, right_factor, (*candidates, far))
    blocks = exchanged(packed.reshape(groups, slots, rows, width), "grp")
    result = products(factors, blocks)
    returned = exchanged(result, "grp").reshape(groups * slots, rows, width)
    homeward = moved(VMEM, outward, returned, columns, "from_slots")
    home = exchanged(homeward, "fsdp")
    return moved(VMEM, landing, home, local_blocks, "from_columns")


def solution(mesh):
    placed = (P("fsdp", "grp", None), P(("fsdp", "grp"), None, None), P(("fsdp", "grp"), None, None), P())
    return jax.shard_map(
        per_device, mesh=mesh, in_specs=placed, out_specs=P("fsdp", "grp", None), check_vma=False
    )
```
